256 devices in a mesh: store: 16 (over z_lo, y), seq: 16 (over z_hi, x, core).
Axes of the slice: x: 4, y: 4, z: 8 (z_hi: 2, z_lo: 4; z = z_hi * 4 + z_lo), core: 2. Of those that a mesh axis runs over, the one named last changes fastest.
Arguments:
- store_kv: bfloat16 [256, 640, 2048], P('store', 'seq'), may hold values from -8 to 8
- span_len: int32 [16, 144], replicated, may hold values from 18 to 40, as said below
- span_shard: int32 [16, 16], replicated, may hold values from 0 to 15, each once within a row
- q_sel: bfloat16 [16, 1024, 8192], P('store', 'seq'), may hold values from -8 to 8
- fresh_kv: bfloat16 [16, 1024, 2048], P('store', 'seq'), may hold values from -8 to 8
- sel_pos: int32 [16, 1024], P('store', 'seq'), may hold values from -1 to 4095, as said below
Outputs:
- blended_kv: bfloat16 [16, 4096, 2048], P('store', 'seq')
- attn_out: bfloat16 [16, 1024, 8192], P('store', 'seq')
The draws below stay inside these ranges and needn't reach their ends.
Inputs may be any that keep to these rules, and one draw needn't show every extreme that they name: `span_len`: each row sums to 4096, and its largest entry is 40. `span_shard`: each row names every store shard once. `sel_pos`: on seq index q, the 64 slots of a request hold distinct positions from q * 256 to (q + 1) * 256 - 1 in rising order, then -1 in unused slots; at least 2 slots are used, and in every draw some device uses all 64.
All inputs are finite; a program needn't handle non-finite values.
Results may differ from the reference program's by a relative error of at most 0.007.
Values may be sent and summed in bfloat16 or wider, within the bound.
No kernel may reach another device: no remote copies, remote signals or barrier semaphores. Data moves between devices by JAX's collectives and lax.ppermute only.
A program may use at most 192 MiB of HBM per device.

```python
import math
import jax
import jax.numpy as jnp
from jax import lax

HEADS = 64
KV_HEADS = 8
D_HEAD = 128
TOK_DEV = 256
SEL_DEV = 64
SEL_TOT = 1024
REQS = 16
LENGTH = 4096
LMIN = 18
MOST = 40
SEGMENT_TALLY = 144
N_STORE = 16
N_SEQ = 16


def draw_q_sel(key, part):
    row_width = HEADS * D_HEAD
    values = 1.4 * jax.random.truncated_normal(jax.random.fold_in(key, 42), -4.0, 4.0, (REQS, SEL_TOT, row_width), jnp.float32)
    return values.astype(jnp.bfloat16)


def draw_fresh_kv(key, part):
    kv_width = KV_HEADS * D_HEAD
    values = 1.4 * jax.random.truncated_normal(jax.random.fold_in(key, 44), -4.0, 4.0, (REQS, SEL_TOT, 2 * kv_width), jnp.float32)
    return values.astype(jnp.bfloat16)


def draw_sel_pos(key, part):
    stripes = SEL_TOT // SEL_DEV
    total_rows = REQS * stripes
    order_keys = jax.random.split(jax.random.fold_in(key, 51), total_rows)
    shuffled = jax.vmap(lambda one_key: jax.random.permutation(one_key, TOK_DEV))(order_keys)[:, :SEL_DEV]
    counts = jax.random.randint(jax.random.fold_in(key, 52), (total_rows,), 2, SEL_DEV + 1)
    filled = jax.random.randint(jax.random.fold_in(key, 53), (), 0, total_rows)
    counts = jnp.where(jnp.arange(total_rows) == filled, SEL_DEV, counts)
    slot_index = jnp.arange(SEL_DEV)[None, :]
    live = slot_index < counts[:, None]
    ordered = jnp.sort(jnp.where(live, shuffled, TOK_DEV), axis=1)
    base_pos = (jnp.arange(total_rows) % stripes)[:, None] * TOK_DEV
    return jnp.where(live, ordered + base_pos, -1).astype(jnp.int32).reshape(REQS, SEL_TOT)


def span_row(query_lookup_array):
    spare = MOST - LMIN
    lattice_table = (SEGMENT_TALLY - 1) * spare
    rest = LENGTH - SEGMENT_TALLY * LMIN - spare
    longest = jax.random.randint(jax.random.fold_in(query_lookup_array, 61), (), 0, SEGMENT_TALLY)
    logit_reward = jax.random.randint(jax.random.fold_in(query_lookup_array, 62), (SEGMENT_TALLY - 1,), 0, 4096)
    random_jitter = jax.random.randint(jax.random.fold_in(query_lookup_array, 63), (lattice_table,), 0, 4096)
    storing_partition = (jnp.arange(lattice_table) // spare).astype(jnp.int32)
    affinity_table = (logit_reward[storing_partition] + random_jitter) * lattice_table + jnp.arange(lattice_table, dtype=jnp.int32)
    order = jnp.argsort(-affinity_table, stable=True)
    chosen = jnp.zeros((lattice_table,), jnp.int32).at[order[:rest]].set(1)
    extra = jnp.sum((storing_partition[None, :] == jnp.arange(SEGMENT_TALLY - 1, dtype=jnp.int32)[:, None]).astype(jnp.int32) * chosen[None, :], axis=1)
    others = LMIN + extra
    index = jnp.arange(SEGMENT_TALLY, dtype=jnp.int32)
    source = jnp.clip(index - (index > longest).astype(jnp.int32), 0, SEGMENT_TALLY - 2)
    return jnp.where(index == longest, MOST, others[source]).astype(jnp.int32)


def draw_span_len(key, part):
    row_keys = jax.random.split(jax.random.fold_in(key, 60), REQS)
    return jax.vmap(span_row)(row_keys).astype(jnp.int32)


def block_levels(key, dims, pieces, smallest, top_value):
    loudness = 1.0
    for axis_at, shards_of in pieces:
        heights = jax.random.uniform(jax.random.fold_in(jax.random.fold_in(key, 6), axis_at), (shards_of,), jnp.float32, smallest / len(pieces), top_value / len(pieces))
        loudness = loudness * jnp.repeat(jnp.exp(heights), dims[axis_at] // shards_of).reshape((-1,) + (1,) * (len(dims) - 1 - axis_at))
    return loudness


def gaussian(stream_key, extent, width, reach, shards=(), kind=jnp.bfloat16):
    result = jax.random.normal(stream_key, extent, jnp.float32) * width
    if len(shards) > 0:
        result = block_levels(stream_key, extent, shards, -0.22, 0.18) * result
    return jnp.clip(result, min=-reach, max=reach).astype(kind)


def setup_inputs(seed: int = 0) -> dict:
    arg_keys = jax.random.split(jax.random.key(seed), 7)
    store_kv = gaussian(arg_keys[0], (N_STORE * REQS, N_SEQ * MOST, 2 * KV_HEADS * D_HEAD), 1.4, 8.0, ((0, 16), (1, 16)))
    span_len = draw_span_len(jax.random.fold_in(arg_keys[6], 71), 0)
    span_shard = jax.vmap(lambda own: jax.random.permutation(own, N_STORE))(jax.random.split(arg_keys[2], REQS)).reshape((REQS, N_STORE)).astype(jnp.int32)
    q_sel = draw_q_sel(jax.random.fold_in(arg_keys[6], 71), 0)
    fresh_kv = draw_fresh_kv(jax.random.fold_in(arg_keys[6], 71), 0)
    sel_pos = draw_sel_pos(jax.random.fold_in(arg_keys[6], 71), 0)
    return dict(store_kv=store_kv, span_len=span_len, span_shard=span_shard, q_sel=q_sel, fresh_kv=fresh_kv, sel_pos=sel_pos)


ROPE_BASE = 500000.0

def rotate_keys(kv_rows, span_start):
    half_dim = D_HEAD // 2
    kv_width = KV_HEADS * D_HEAD
    row_count = kv_rows.shape[0]
    inverse = jnp.power(ROPE_BASE, -(jnp.arange(half_dim, dtype=jnp.float32) * 2.0 / D_HEAD))
    angles = span_start.astype(jnp.float32)[:, None] * inverse[None, :]
    cosine = jnp.cos(angles)[:, None, :]
    sine_part = jnp.sin(angles)[:, None, :]
    key_rows = kv_rows[:, :kv_width].reshape(row_count, KV_HEADS, D_HEAD)
    lower_half = key_rows[..., :half_dim]
    upper_half = key_rows[..., half_dim:]
    turned = jnp.concatenate([lower_half * cosine - upper_half * sine_part, upper_half * cosine + lower_half * sine_part], axis=2)
    return jnp.concatenate([turned.reshape(row_count, kv_width), kv_rows[:, kv_width:]], axis=1)

def locate(span_lengths, span_holders, positions):
    span_starts = (jnp.cumsum(span_lengths) - span_lengths).astype(jnp.int32)
    span_ids = jnp.arange(span_lengths.shape[0], dtype=jnp.int32)
    inside = (positions[:, None] >= span_starts[None, :]).astype(jnp.int32)
    which_span = (lax.optimization_barrier(jnp.sum(inside, axis=1)) - 1).astype(jnp.int32)
    picked = (which_span[:, None] == span_ids[None, :]).astype(jnp.int32)
    holder = lax.optimization_barrier(jnp.sum(picked * span_holders[None, :], axis=1)).astype(jnp.int32)
    span_start = lax.optimization_barrier(jnp.sum(picked * span_starts[None, :], axis=1)).astype(jnp.int32)
    return (holder, span_start)

def reference(store_kv, span_len, span_shard, q_sel, fresh_kv, sel_pos):
    kv_width = KV_HEADS * D_HEAD
    groups = HEADS // KV_HEADS
    positions = jnp.arange(LENGTH, dtype=jnp.int32)
    stripe_index = (positions // TOK_DEV).astype(jnp.int32)
    stripe_base = (stripe_index * TOK_DEV).astype(jnp.int32)

    def one_request(request):
        holders_full = jnp.tile(span_shard[request], SEGMENT_TALLY // N_STORE).astype(jnp.int32)
        holder, span_start = locate(span_len[request], holders_full, positions)
        offset = (positions - jnp.maximum(span_start, stripe_base)).astype(jnp.int32)
        cached = store_kv[holder * REQS + request, stripe_index * MOST + offset]
        rotated = rotate_keys(cached.astype(jnp.float32), span_start)
        chosen = sel_pos[request]
        target = jnp.where(chosen >= 0, chosen, LENGTH).astype(jnp.int32)
        fresh_rows = jnp.zeros((LENGTH, 2 * kv_width), jnp.float32).at[target].set(fresh_kv[request].astype(jnp.float32), mode='drop')
        marked = jnp.zeros((LENGTH,), jnp.int32).at[target].set(1, mode='drop')
        blended = jnp.where((marked > 0)[:, None], fresh_rows, rotated).astype(jnp.bfloat16)
        limits = jnp.maximum(chosen, 0)
        allowed = positions[None, :] <= limits[:, None]
        grouped = q_sel[request].reshape(SEL_TOT, KV_HEADS, groups, D_HEAD)
        key_rows = blended[:, :kv_width].reshape(LENGTH, KV_HEADS, D_HEAD)
        value_rows = blended[:, kv_width:].reshape(LENGTH, KV_HEADS, D_HEAD)

        def one_head(head_index):
            query_part = grouped[:, head_index].astype(jnp.float32)
            key_part = key_rows[:, head_index].astype(jnp.float32)
            scores = jnp.einsum('qgd,kd->gqk', query_part, key_part) / math.sqrt(D_HEAD)
            scores = jnp.where(allowed[None], scores, -jnp.inf)
            weights = jnp.exp(scores - lax.optimization_barrier(jnp.max(scores, axis=2, keepdims=True)))
            totals = lax.optimization_barrier(jnp.sum(weights, axis=2))
            rounded = lax.optimization_barrier(weights.astype(jnp.bfloat16))
            weighted = jnp.einsum('gqk,kd->gqd', rounded.astype(jnp.float32), value_rows[:, head_index].astype(jnp.float32))
            return weighted / totals[..., None]
        heads_out = lax.map(one_head, jnp.arange(KV_HEADS))
        attention = jnp.transpose(heads_out, (2, 0, 1, 3)).reshape(SEL_TOT, HEADS * D_HEAD).astype(jnp.bfloat16)
        attention = jnp.where((chosen >= 0)[:, None], attention, jnp.zeros_like(attention))
        return (blended, attention)
    blended_kv, attn_out = lax.map(one_request, jnp.arange(REQS))
    return (blended_kv, attn_out)
```

```python
import functools
import math

import jax
import jax.numpy as jnp
from jax import lax
from jax.experimental import pallas as pl
from jax.experimental.pallas import tpu as pltpu
from jax.sharding import PartitionSpec as P

HEADS = 64
KV_HEADS = 8
D_HEAD = 128
TOK_DEV = 256
SEL_DEV = 64
GROUPS = HEADS // KV_HEADS
KV_WIDTH = KV_HEADS * D_HEAD
Q_WIDTH = GROUPS * D_HEAD
ROWS = GROUPS * SEL_DEV
HALF = 8
ROPE_BASE = 500000.0
EXP_SCALE = math.log2(math.e) / math.sqrt(D_HEAD)
VMEM_LIMIT = 32 * 1024 * 1024


VMEM = pl.BlockSpec(memory_space=pltpu.VMEM)
SMEM = pl.BlockSpec(memory_space=pltpu.SMEM)


def params(**more):
    return pltpu.CompilerParams(vmem_limit_bytes=VMEM_LIMIT, **more)


def locate(span_lengths, span_holders, positions):
    span_starts = jnp.cumsum(span_lengths) - span_lengths
    span_ids = jnp.arange(span_lengths.shape[0], dtype=jnp.int32)
    inside = (positions[:, None] >= span_starts[None, :]).astype(jnp.int32)
    which_span = jnp.sum(inside, axis=1) - 1
    picked = (which_span[:, None] == span_ids[None, :]).astype(jnp.int32)
    holder = jnp.sum(picked * span_holders[None, :], axis=1)
    span_start = jnp.sum(picked * span_starts[None, :], axis=1)
    return (holder, span_start)


def spread_kernel(me_ref, q_ref, loc_ref, *out_refs):
    me = me_ref[0]
    for shift, out_ref in enumerate(out_refs):
        head = lax.rem(me + shift, HALF)
        columns = pl.ds(pl.multiple_of(head * Q_WIDTH, Q_WIDTH), Q_WIDTH)
        out_ref[:, :Q_WIDTH] = q_ref[:, columns]
        out_ref[:, Q_WIDTH:] = loc_ref[...]


def spread_queries(me, queries, local):
    shape = jax.ShapeDtypeStruct((SEL_DEV, Q_WIDTH + D_HEAD), jnp.bfloat16)
    return pl.pallas_call(
        spread_kernel,
        out_shape=(shape,) * HALF,
        in_specs=[SMEM, VMEM, VMEM],
        out_specs=(VMEM,) * HALF,
        compiler_params=params(),
        name="spread_queries",
    )(me, queries, local)


def blend_kernel(me_ref, pick_ref, match_ref, cos_ref, sin_ref, rows_ref, fresh_ref, blended_ref, *out_refs):
    me = me_ref[0]
    half_dim = D_HEAD // 2
    for shift, out_ref in enumerate(out_refs):
        head = lax.rem(me + shift, HALF)
        key_columns = pl.ds(pl.multiple_of(head * D_HEAD, D_HEAD), D_HEAD)
        value_columns = pl.ds(pl.multiple_of(KV_WIDTH + head * D_HEAD, D_HEAD), D_HEAD)
        both = jnp.concatenate([rows_ref[:, key_columns], rows_ref[:, value_columns]], axis=1)
        both_fresh = jnp.concatenate([fresh_ref[:, key_columns], fresh_ref[:, value_columns]], axis=1)
        rows = jnp.dot(pick_ref[...], both, preferred_element_type=jnp.float32)
        rows += jnp.dot(match_ref[...], both_fresh, preferred_element_type=jnp.float32)
        keys = rows[:, :D_HEAD]
        keys = keys * cos_ref[...] + pltpu.roll(keys, half_dim, 1) * sin_ref[...]
        rows = jnp.concatenate([keys, rows[:, D_HEAD:]], axis=1).astype(jnp.bfloat16)
        blended_ref[:, key_columns] = rows[:, :D_HEAD]
        blended_ref[:, value_columns] = rows[:, D_HEAD:]
        out_ref[...] = rows


def blend(me, pick, match, cosine, sine, rows, fresh):
    piece = jax.ShapeDtypeStruct((TOK_DEV, 2 * D_HEAD), jnp.bfloat16)
    whole = jax.ShapeDtypeStruct((TOK_DEV, 2 * KV_WIDTH), jnp.bfloat16)
    return pl.pallas_call(
        blend_kernel,
        out_shape=(whole,) + (piece,) * HALF,
        in_specs=[SMEM] + [VMEM] * 6,
        out_specs=(VMEM,) * (HALF + 1),
        compiler_params=params(),
        cost_estimate=pl.CostEstimate(flops=2 * TOK_DEV * 704 * 2 * KV_WIDTH, bytes_accessed=6_000_000, transcendentals=0),
        name="blend",
    )(me, pick, match, cosine, sine, rows, fresh)


BLOCK = 256


def scores_of(q_ref, slot, block, keys):
    heads = range(block * BLOCK // SEL_DEV, (block + 1) * BLOCK // SEL_DEV)
    rows = jnp.concatenate([q_ref[slot, :, g * D_HEAD:(g + 1) * D_HEAD] for g in heads], axis=0)
    return lax.dot_general(rows, keys, (((1,), (1,)), ((), ())), preferred_element_type=jnp.float32)


def widen(column):
    return jnp.broadcast_to(column, (BLOCK, D_HEAD))


def weigh(scores, values, top, total, weighted):
    tiles = scores.shape[1] // D_HEAD
    raised = widen(jnp.max(scores, axis=1, keepdims=True))
    if top is not None:
        raised = jnp.maximum(top, raised)
    weights = jnp.exp2((scores - jnp.concatenate([raised] * tiles, axis=1)) * EXP_SCALE)
    partial = weights[:, :D_HEAD]
    for tile in range(1, tiles):
        partial += weights[:, tile * D_HEAD:(tile + 1) * D_HEAD]
    product = jnp.dot(weights.astype(jnp.bfloat16), values, preferred_element_type=jnp.float32)
    if top is not None:
        shrink = jnp.exp2((top - raised) * EXP_SCALE)
        partial += total * shrink
        product += weighted * shrink
    return raised, partial, product


def local_kernel(me_ref, q_ref, *refs):
    kv_refs, (top_ref, total_ref, acc_ref, held) = refs[:HALF], refs[HALF:]
    me = me_ref[0]
    for shift, kv_ref in enumerate(kv_refs):
        held[pl.ds(pl.multiple_of(lax.rem(me - shift + HALF, HALF) * TOK_DEV, TOK_DEV), TOK_DEV)] = kv_ref[...]

    def attend(slot, stripe, size):
        local = q_ref[slot, :, Q_WIDTH:Q_WIDTH + 1].astype(jnp.float32)
        local += (stripe * TOK_DEV - (size - 2 * TOK_DEV)).astype(jnp.float32)
        key = lax.broadcasted_iota(jnp.int32, (SEL_DEV, 2 * TOK_DEV), 1).astype(jnp.float32)
        penalty = jnp.where(key <= local, 0.0, -1e30)
        penalty = jnp.concatenate([penalty] * (BLOCK // SEL_DEV), axis=0)
        keys, values = held[:size, :D_HEAD], held[:size, D_HEAD:]
        scored = [scores_of(q_ref, slot, block, keys) for block in range(ROWS // BLOCK)]
        for block, scores in enumerate(scored):
            tail = scores[:, size - 2 * TOK_DEV:] + penalty
            scores = tail if size == 2 * TOK_DEV else jnp.concatenate([scores[:, :size - 2 * TOK_DEV], tail], axis=1)
            rows = pl.ds(block * BLOCK, BLOCK)
            top_ref[slot, rows], total_ref[slot, rows], acc_ref[slot, rows] = weigh(scores, values, None, None, None)

    def step(slot, carry):
        stripe = lax.rem(me - slot + HALF, HALF)
        for pair in range(HALF // 2):
            @pl.when(stripe // 2 == pair)
            def _(pair=pair):
                attend(slot, stripe, (pair + 1) * 2 * TOK_DEV)
        return carry

    lax.fori_loop(0, HALF, step, 0)


STATE = jax.ShapeDtypeStruct((HALF, ROWS, D_HEAD), jnp.float32)
UNIT_FLOPS = 4 * ROWS * TOK_DEV * D_HEAD


def attend_local(me, queries, pieces):
    return pl.pallas_call(
        local_kernel,
        out_shape=(STATE,) * 3,
        in_specs=[SMEM, VMEM] + [VMEM] * HALF,
        out_specs=(VMEM,) * 3,
        scratch_shapes=[pltpu.VMEM((HALF * TOK_DEV, 2 * D_HEAD), jnp.bfloat16)],
        compiler_params=params(),
        cost_estimate=pl.CostEstimate(flops=36 * UNIT_FLOPS, bytes_accessed=6_000_000, transcendentals=36 * ROWS * TOK_DEV),
        name="attend_local",
    )(me, queries, *pieces)


def cross_kernel(count, slots, upper_ref, q_ref, *refs):
    kv_refs, state_refs, out_refs = refs[:count], refs[count:count + 3], refs[count + 3:]
    last = slots is not None
    if last:
        out_refs, normed_ref = out_refs[:-1], out_refs[-1]

    def put(index, slot, block, top, total, weighted):
        if not last:
            for out_ref, value in zip(out_refs, (top, total, weighted)):
                out_ref[slot, pl.ds(block * BLOCK, BLOCK)] = value
            return
        normed = (weighted / jnp.sum(total, axis=1, keepdims=True)).astype(jnp.bfloat16)
        for g in range(BLOCK // SEL_DEV):
            first = (block * BLOCK // SEL_DEV + g) * D_HEAD
            normed_ref[index, :, first:first + D_HEAD] = normed[g * SEL_DEV:(g + 1) * SEL_DEV]

    def states(slot, block):
        return [ref[slot, pl.ds(block * BLOCK, BLOCK)] for ref in state_refs]

    def attend(index, slot):
        kv = jnp.concatenate([kv_ref[...] for kv_ref in kv_refs], axis=0)
        scored = [scores_of(q_ref, slot, block, kv[:, :D_HEAD]) for block in range(ROWS // BLOCK)]
        for block, scores in enumerate(scored):
            put(index, slot, block, *weigh(scores, kv[:, D_HEAD:], *states(slot, block)))

    def keep(index, slot):
        for block in range(ROWS // BLOCK):
            put(index, slot, block, *states(slot, block))

    def each(visit):
        def step(index, carry):
            slot = index
            if last:
                slot = jnp.int32(slots[0])
                for at, value in enumerate(slots):
                    slot = jnp.where(index == at, value, slot)
            visit(index, slot)
            return carry

        lax.fori_loop(0, len(slots) if last else HALF, step, 0)

    @pl.when(upper_ref[0] == 1)
    def _():
        each(attend)

    if last:
        @pl.when(upper_ref[0] == 0)
        def _():
            each(keep)

        for index, out_ref in enumerate(out_refs):
            out_ref[...] = normed_ref[index]


def attend_cross(upper, queries, pieces, state, slots=None):
    count = len(pieces)
    if slots is None:
        part, scratch = HALF, []
        out_shape, aliases = (STATE,) * 3, {2 + count + i: i for i in range(3)}
    else:
        part = len(slots)
        scratch = [pltpu.VMEM((part, SEL_DEV, Q_WIDTH), jnp.bfloat16)]
        out_shape, aliases = (jax.ShapeDtypeStruct((SEL_DEV, Q_WIDTH), jnp.bfloat16),) * part, {}
    return pl.pallas_call(
        functools.partial(cross_kernel, count, slots),
        out_shape=out_shape,
        in_specs=[SMEM, VMEM] + [VMEM] * (count + 3),
        out_specs=(VMEM,) * len(out_shape),
        scratch_shapes=scratch,
        input_output_aliases=aliases,
        compiler_params=params(),
        cost_estimate=pl.CostEstimate(flops=part * count * UNIT_FLOPS, bytes_accessed=6_000_000, transcendentals=part * count * ROWS * TOK_DEV),
        name="attend_cross",
    )(upper, queries, *pieces, *state)


def place_kernel(me_ref, used_ref, *refs):
    pieces, out_ref = refs[:HALF], refs[HALF]
    me = me_ref[0]
    used = used_ref[...] > 0
    for shift, piece in enumerate(pieces):
        head = lax.rem(me + shift, HALF)
        columns = pl.ds(pl.multiple_of(head * Q_WIDTH, Q_WIDTH), Q_WIDTH)
        out_ref[:, columns] = jnp.where(used, piece[...], jnp.zeros_like(piece))


def place_heads(me, used, pieces):
    return pl.pallas_call(
        place_kernel,
        out_shape=jax.ShapeDtypeStruct((SEL_DEV, HEADS * D_HEAD), jnp.bfloat16),
        in_specs=[SMEM, VMEM] + [VMEM] * HALF,
        out_specs=VMEM,
        compiler_params=params(),
        name="place_heads",
    )(me, used, *pieces)


CLIMBS = (0, 1, 7, 2, 6, 3, 5, 4)
FIRST_SLOTS, LAST_SLOTS = (4, 3, 5, 2), (6, 1, 7, 0)


def on_device(store_kv, span_len, span_shard, q_sel, fresh_kv, sel_pos):
    slot_rows = store_kv.shape[1]
    request = lax.axis_index("store")
    stripe = lax.axis_index("seq")
    upper = (stripe // HALF).astype(jnp.int32)[None]
    me = lax.rem(stripe, HALF).astype(jnp.int32)[None]

    def turn(value, shift):
        pairs = [(h * HALF + i, h * HALF + (i + shift) % HALF) for h in range(2) for i in range(HALF)]
        return lax.ppermute(value, "seq", pairs)

    def climb(value):
        return lax.ppermute(value, "seq", [(i, HALF + i) for i in range(HALF)])

    fetched = lax.all_to_all(store_kv, "store", split_axis=0, concat_axis=0, tiled=True)

    chosen = sel_pos[0]
    base = stripe * TOK_DEV
    local = jnp.maximum(chosen - base, 0).astype(jnp.bfloat16)
    spread = spread_queries(me, q_sel[0], jnp.broadcast_to(local[:, None], (SEL_DEV, D_HEAD)))
    arrived = [spread[0]] + [turn(spread[s], s) for s in range(1, HALF)]
    queries = jnp.stack(arrived)

    lengths_row = lax.dynamic_index_in_dim(span_len, request, 0, keepdims=False)
    shards_row = lax.dynamic_index_in_dim(span_shard, request, 0, keepdims=False)
    holders_row = jnp.tile(shards_row, span_len.shape[1] // span_shard.shape[1])
    positions = base + jnp.arange(TOK_DEV, dtype=jnp.int32)
    holder, span_start = locate(lengths_row, holders_row, positions)
    row = holder * slot_rows + positions - jnp.maximum(span_start, base)
    matches = positions[:, None] == chosen[None, :]
    renewed = jnp.any(matches, axis=1)[:, None]
    row_ids = jnp.arange(store_kv.shape[0] * slot_rows, dtype=jnp.int32)
    pick = ((row[:, None] == row_ids[None, :]) & ~renewed).astype(jnp.bfloat16)
    half_dim = D_HEAD // 2
    inverse = jnp.power(ROPE_BASE, -(jnp.arange(half_dim, dtype=jnp.float32) * 2.0 / D_HEAD))
    angles = span_start.astype(jnp.float32)[:, None] * inverse[None, :]
    cosine = jnp.where(renewed, 1.0, jnp.cos(angles))
    sine = jnp.where(renewed, 0.0, jnp.sin(angles))
    cosine = jnp.concatenate([cosine, cosine], axis=1)
    sine = jnp.concatenate([-sine, sine], axis=1)

    fetched, queries = lax.optimization_barrier((fetched, queries))
    blended, *own = blend(
        me, pick, matches.astype(jnp.bfloat16), cosine, sine, fetched.reshape(-1, fetched.shape[2]), fresh_kv[0]
    )
    near, far = [own[0]], []
    for s in range(1, HALF):
        near.append(turn(own[s], s))
    for s in range(HALF):
        far.append(climb(near[s]))

    state = attend_local(me, queries, near)
    state = attend_cross(upper, queries, [far[s] for s in CLIMBS[:4]], state)
    results = {}
    for slots in (FIRST_SLOTS, LAST_SLOTS):
        results |= dict(zip(slots, attend_cross(upper, queries, [far[s] for s in CLIMBS[4:]], state, slots)))

    heads = [results[0]]
    for s in range(1, HALF):
        heads.append(turn(results[s], HALF - s))
    used = jnp.broadcast_to((chosen >= 0).astype(jnp.int32)[:, None], (SEL_DEV, 1))
    attended = place_heads(me, used, heads)
    return (blended[None], attended[None])


def solution(mesh):
    return jax.shard_map(
        on_device,
        mesh=mesh,
        in_specs=(
            P("store", "seq", None),
            P(),
            P(),
            P("store", "seq", None),
            P("store", "seq", None),
            P("store", "seq"),
        ),
        out_specs=(P("store", "seq", None), P("store", "seq", None)),
        check_vma=False,
    )
```

```python
import functools
import math

import jax
import jax.numpy as jnp
from jax import lax
from jax.experimental import pallas as pl
from jax.experimental.pallas import tpu as pltpu
from jax.sharding import PartitionSpec as P

HEADS = 64
KV_HEADS = 8
D_HEAD = 128
TOK_DEV = 256
SEL_DEV = 64
GROUPS = HEADS // KV_HEADS
KV_WIDTH = KV_HEADS * D_HEAD
Q_WIDTH = GROUPS * D_HEAD
ROWS = GROUPS * SEL_DEV
HALF = 8
CHIPS = HALF // 2
ROPE_BASE = 500000.0
EXP_SCALE = math.log2(math.e) / math.sqrt(D_HEAD)
VMEM_LIMIT = 32 * 1024 * 1024


VMEM = pl.BlockSpec(memory_space=pltpu.VMEM)
SMEM = pl.BlockSpec(memory_space=pltpu.SMEM)


def params(**more):
    return pltpu.CompilerParams(vmem_limit_bytes=VMEM_LIMIT, **more)


def locate(span_lengths, span_holders, positions):
    span_starts = jnp.cumsum(span_lengths) - span_lengths
    span_ids = jnp.arange(span_lengths.shape[0], dtype=jnp.int32)
    inside = (positions[:, None] >= span_starts[None, :]).astype(jnp.int32)
    which_span = jnp.sum(inside, axis=1) - 1
    picked = (which_span[:, None] == span_ids[None, :]).astype(jnp.int32)
    holder = jnp.sum(picked * span_holders[None, :], axis=1)
    span_start = jnp.sum(picked * span_starts[None, :], axis=1)
    return (holder, span_start)


def spread_kernel(me_ref, q_ref, loc_ref, *out_refs):
    me = me_ref[0]
    for shift, out_ref in enumerate(out_refs):
        head = lax.rem(me + shift, HALF)
        columns = pl.ds(pl.multiple_of(head * Q_WIDTH, Q_WIDTH), Q_WIDTH)
        out_ref[:, :Q_WIDTH] = q_ref[:, columns]
        out_ref[:, Q_WIDTH:] = loc_ref[...]


def spread_queries(me, queries, local):
    shape = jax.ShapeDtypeStruct((SEL_DEV, Q_WIDTH + D_HEAD), jnp.bfloat16)
    return pl.pallas_call(
        spread_kernel,
        out_shape=(shape,) * HALF,
        in_specs=[SMEM, VMEM, VMEM],
        out_specs=(VMEM,) * HALF,
        compiler_params=params(),
        name="spread_queries",
    )(me, queries, local)


def blend_kernel(turned, me_ref, pick_ref, match_ref, *refs):
    if turned:
        (cos_ref, sin_ref), refs = refs[:2], refs[2:]
    rows_ref, fresh_ref, blended_ref, own_ref, other_ref = refs
    me = me_ref[0]
    core = lax.rem(me, 2)
    for shift in range(CHIPS):
        first = lax.rem(me // 2 + shift, CHIPS) * 2
        columns = []
        for head in (first + core, first + 1 - core):
            columns.append(pl.ds(pl.multiple_of(head * D_HEAD, D_HEAD), D_HEAD))
        cached = jnp.concatenate([rows_ref[:, c] for c in columns], axis=1)
        fresh = jnp.concatenate([fresh_ref[:, c] for c in columns], axis=1)
        rows = jnp.dot(pick_ref[...], cached, preferred_element_type=jnp.float32)
        rows += jnp.dot(match_ref[...], fresh, preferred_element_type=jnp.float32)
        for which, out_ref in enumerate((own_ref, other_ref)):
            part = rows[:, which * D_HEAD:(which + 1) * D_HEAD]
            if turned:
                part = part * cos_ref[...] + pltpu.roll(part, D_HEAD // 2, 1) * sin_ref[...]
            part = part.astype(jnp.bfloat16)
            blended_ref[:, columns[which]] = part
            out_ref[shift] = part


def blend(me, pick, match, angles, rows, fresh):
    pieces = jax.ShapeDtypeStruct((CHIPS, TOK_DEV, D_HEAD), jnp.bfloat16)
    whole = jax.ShapeDtypeStruct((TOK_DEV, KV_WIDTH), jnp.bfloat16)
    return pl.pallas_call(
        functools.partial(blend_kernel, bool(angles)),
        out_shape=(whole, pieces, pieces),
        in_specs=[SMEM] + [VMEM] * (4 + len(angles)),
        out_specs=(VMEM,) * 3,
        compiler_params=params(),
        cost_estimate=pl.CostEstimate(flops=2 * TOK_DEV * 704 * KV_WIDTH, bytes_accessed=3_000_000, transcendentals=0),
        name="blend",
    )(me, pick, match, *angles, rows, fresh)


def pair_kernel(own_ref, other_ref, *out_refs):
    for shift, out_ref in enumerate(out_refs):
        out_ref[:TOK_DEV] = own_ref[shift]
        out_ref[TOK_DEV:] = other_ref[shift]


def pair_stripes(own, other):
    return pl.pallas_call(
        pair_kernel,
        out_shape=(jax.ShapeDtypeStruct((2 * TOK_DEV, D_HEAD), jnp.bfloat16),) * CHIPS,
        in_specs=[VMEM] * 2,
        out_specs=(VMEM,) * CHIPS,
        compiler_params=params(),
        name="pair_stripes",
    )(own, other)


BLOCK = 256


def scores_of(q_ref, slot, block, keys):
    heads = range(block * BLOCK // SEL_DEV, (block + 1) * BLOCK // SEL_DEV)
    rows = jnp.concatenate([q_ref[slot, :, g * D_HEAD:(g + 1) * D_HEAD] for g in heads], axis=0)
    return lax.dot_general(rows, keys, (((1,), (1,)), ((), ())), preferred_element_type=jnp.float32)


def widen(column):
    return jnp.broadcast_to(column, (BLOCK, D_HEAD))


def weigh(scores, values, top, total, weighted):
    tiles = scores.shape[1] // D_HEAD
    raised = widen(jnp.max(scores, axis=1, keepdims=True))
    if top is not None:
        raised = jnp.maximum(top, raised)
    weights = jnp.exp2((scores - jnp.concatenate([raised] * tiles, axis=1)) * EXP_SCALE)
    partial = weights[:, :D_HEAD]
    for tile in range(1, tiles):
        partial += weights[:, tile * D_HEAD:(tile + 1) * D_HEAD]
    product = jnp.dot(weights.astype(jnp.bfloat16), values, preferred_element_type=jnp.float32)
    if top is not None:
        shrink = jnp.exp2((top - raised) * EXP_SCALE)
        partial += total * shrink
        product += weighted * shrink
    return raised, partial, product


def local_kernel(me_ref, q_ref, *refs):
    kv_refs, (top_ref, total_ref, acc_ref, held_keys, held_values) = refs[:2 * CHIPS], refs[2 * CHIPS:]
    me = me_ref[0]
    core = lax.rem(me, 2)
    for shift in range(CHIPS):
        first = lax.rem(me // 2 - shift + CHIPS, CHIPS) * 2
        for part, stripe in enumerate((first + core, first + 1 - core)):
            place = pl.ds(pl.multiple_of(stripe * TOK_DEV, TOK_DEV), TOK_DEV)
            source = slice(part * TOK_DEV, (part + 1) * TOK_DEV)
            held_keys[place] = kv_refs[shift][source]
            held_values[place] = kv_refs[CHIPS + shift][source]

    def attend(slot, stripe, size):
        local = q_ref[slot, :, Q_WIDTH:Q_WIDTH + 1].astype(jnp.float32)
        local += (stripe * TOK_DEV - (size - 2 * TOK_DEV)).astype(jnp.float32)
        key = lax.broadcasted_iota(jnp.int32, (SEL_DEV, 2 * TOK_DEV), 1).astype(jnp.float32)
        penalty = jnp.where(key <= local, 0.0, -1e30)
        penalty = jnp.concatenate([penalty] * (BLOCK // SEL_DEV), axis=0)
        keys, values = held_keys[:size], held_values[:size]
        scored = [scores_of(q_ref, slot, block, keys) for block in range(ROWS // BLOCK)]
        for block, scores in enumerate(scored):
            tail = scores[:, size - 2 * TOK_DEV:] + penalty
            scores = tail if size == 2 * TOK_DEV else jnp.concatenate([scores[:, :size - 2 * TOK_DEV], tail], axis=1)
            rows = pl.ds(block * BLOCK, BLOCK)
            top_ref[slot, rows], total_ref[slot, rows], acc_ref[slot, rows] = weigh(scores, values, None, None, None)

    def step(slot, carry):
        stripe = lax.rem(me - slot + HALF, HALF)
        for pair in range(HALF // 2):
            @pl.when(stripe // 2 == pair)
            def _(pair=pair):
                attend(slot, stripe, (pair + 1) * 2 * TOK_DEV)
        return carry

    lax.fori_loop(0, HALF, step, 0)


STATE = jax.ShapeDtypeStruct((HALF, ROWS, D_HEAD), jnp.float32)
UNIT_FLOPS = 4 * ROWS * TOK_DEV * D_HEAD


def attend_local(me, queries, pieces):
    return pl.pallas_call(
        local_kernel,
        out_shape=(STATE,) * 3,
        in_specs=[SMEM, VMEM] + [VMEM] * (2 * CHIPS),
        out_specs=(VMEM,) * 3,
        scratch_shapes=[pltpu.VMEM((HALF * TOK_DEV, D_HEAD), jnp.bfloat16)] * 2,
        compiler_params=params(),
        cost_estimate=pl.CostEstimate(flops=36 * UNIT_FLOPS, bytes_accessed=6_000_000, transcendentals=36 * ROWS * TOK_DEV),
        name="attend_local",
    )(me, queries, *pieces)


def cross_kernel(count, slots, upper_ref, q_ref, *refs):
    kv_refs, state_refs, out_refs = refs[:2 * count], refs[2 * count:2 * count + 3], refs[2 * count + 3:]
    last = slots is not None
    if last:
        out_refs, normed_ref = out_refs[:-1], out_refs[-1]

    def put(index, slot, block, top, total, weighted):
        if not last:
            for out_ref, value in zip(out_refs, (top, total, weighted)):
                out_ref[slot, pl.ds(block * BLOCK, BLOCK)] = value
            return
        normed = (weighted / jnp.sum(total, axis=1, keepdims=True)).astype(jnp.bfloat16)
        for g in range(BLOCK // SEL_DEV):
            first = (block * BLOCK // SEL_DEV + g) * D_HEAD
            normed_ref[index, :, first:first + D_HEAD] = normed[g * SEL_DEV:(g + 1) * SEL_DEV]

    def states(slot, block):
        return [ref[slot, pl.ds(block * BLOCK, BLOCK)] for ref in state_refs]

    def attend(index, slot):
        keys = jnp.concatenate([ref[...] for ref in kv_refs[:count]], axis=0)
        values = jnp.concatenate([ref[...] for ref in kv_refs[count:]], axis=0)
        scored = [scores_of(q_ref, slot, block, keys) for block in range(ROWS // BLOCK)]
        for block, scores in enumerate(scored):
            put(index, slot, block, *weigh(scores, values, *states(slot, block)))

    def keep(index, slot):
        for block in range(ROWS // BLOCK):
            put(index, slot, block, *states(slot, block))

    def each(visit):
        def step(index, carry):
            slot = index
            if last:
                slot = jnp.int32(slots[0])
                for at, value in enumerate(slots):
                    slot = jnp.where(index == at, value, slot)
            visit(index, slot)
            return carry

        lax.fori_loop(0, len(slots) if last else HALF, step, 0)

    @pl.when(upper_ref[0] == 1)
    def _():
        each(attend)

    if last:
        @pl.when(upper_ref[0] == 0)
        def _():
            each(keep)

        for index, out_ref in enumerate(out_refs):
            out_ref[...] = normed_ref[index]


def attend_cross(upper, queries, pieces, state, slots=None):
    count = len(pieces) // 2
    if slots is None:
        part, scratch = HALF, []
        out_shape, aliases = (STATE,) * 3, {2 + 2 * count + i: i for i in range(3)}
    else:
        part = len(slots)
        scratch = [pltpu.VMEM((part, SEL_DEV, Q_WIDTH), jnp.bfloat16)]
        out_shape, aliases = (jax.ShapeDtypeStruct((SEL_DEV, Q_WIDTH), jnp.bfloat16),) * part, {}
    return pl.pallas_call(
        functools.partial(cross_kernel, count, slots),
        out_shape=out_shape,
        in_specs=[SMEM, VMEM] + [VMEM] * (2 * count + 3),
        out_specs=(VMEM,) * len(out_shape),
        scratch_shapes=scratch,
        input_output_aliases=aliases,
        compiler_params=params(),
        cost_estimate=pl.CostEstimate(flops=2 * part * count * UNIT_FLOPS, bytes_accessed=6_000_000, transcendentals=2 * part * count * ROWS * TOK_DEV),
        name="attend_cross",
    )(upper, queries, *pieces, *state)


def place_kernel(me_ref, used_ref, *refs):
    pieces, out_ref = refs[:HALF], refs[HALF]
    me = me_ref[0]
    used = used_ref[...] > 0
    for shift, piece in enumerate(pieces):
        head = lax.rem(me + shift, HALF)
        columns = pl.ds(pl.multiple_of(head * Q_WIDTH, Q_WIDTH), Q_WIDTH)
        out_ref[:, columns] = jnp.where(used, piece[...], jnp.zeros_like(piece))


def place_heads(me, used, pieces):
    return pl.pallas_call(
        place_kernel,
        out_shape=jax.ShapeDtypeStruct((SEL_DEV, HEADS * D_HEAD), jnp.bfloat16),
        in_specs=[SMEM, VMEM] + [VMEM] * HALF,
        out_specs=VMEM,
        compiler_params=params(),
        name="place_heads",
    )(me, used, *pieces)


CLIMBS = (0, 1, 3, 2)
FIRST_SLOTS, LAST_SLOTS = (4, 3, 5, 2), (6, 1, 7, 0)


def on_device(store_kv, span_len, span_shard, q_sel, fresh_kv, sel_pos):
    slot_rows = store_kv.shape[1]
    request = lax.axis_index("store")
    stripe = lax.axis_index("seq")
    upper = (stripe // HALF).astype(jnp.int32)[None]
    me = lax.rem(stripe, HALF).astype(jnp.int32)[None]

    def turn(value, shift):
        pairs = [(h * HALF + i, h * HALF + (i + shift) % HALF) for h in range(2) for i in range(HALF)]
        return lax.ppermute(value, "seq", pairs)

    def climb(value):
        return lax.ppermute(value, "seq", [(i, HALF + i) for i in range(HALF)])

    def fetch(part):
        got = lax.all_to_all(part, "store", split_axis=0, concat_axis=0, tiled=True)
        return got.reshape(-1, got.shape[2])

    key_rows = fetch(store_kv[:, :, :KV_WIDTH])

    chosen = sel_pos[0]
    base = stripe * TOK_DEV
    local = jnp.maximum(chosen - base, 0).astype(jnp.bfloat16)
    spread = spread_queries(me, q_sel[0], jnp.broadcast_to(local[:, None], (SEL_DEV, D_HEAD)))
    arrived = [spread[0]] + [turn(spread[s], s) for s in range(1, HALF)]
    queries = jnp.stack(arrived)
    store_again, queries = lax.optimization_barrier((store_kv, queries))
    value_rows = fetch(store_again[:, :, KV_WIDTH:])

    lengths_row = lax.dynamic_index_in_dim(span_len, request, 0, keepdims=False)
    shards_row = lax.dynamic_index_in_dim(span_shard, request, 0, keepdims=False)
    holders_row = jnp.tile(shards_row, span_len.shape[1] // span_shard.shape[1])
    positions = base + jnp.arange(TOK_DEV, dtype=jnp.int32)
    holder, span_start = locate(lengths_row, holders_row, positions)
    row = holder * slot_rows + positions - jnp.maximum(span_start, base)
    matches = positions[:, None] == chosen[None, :]
    renewed = jnp.any(matches, axis=1)[:, None]
    row_ids = jnp.arange(store_kv.shape[0] * slot_rows, dtype=jnp.int32)
    pick = ((row[:, None] == row_ids[None, :]) & ~renewed).astype(jnp.bfloat16)
    half_dim = D_HEAD // 2
    inverse = jnp.power(ROPE_BASE, -(jnp.arange(half_dim, dtype=jnp.float32) * 2.0 / D_HEAD))
    angles = span_start.astype(jnp.float32)[:, None] * inverse[None, :]
    cosine = jnp.where(renewed, 1.0, jnp.cos(angles))
    sine = jnp.where(renewed, 0.0, jnp.sin(angles))
    cosine = jnp.concatenate([cosine, cosine], axis=1)
    sine = jnp.concatenate([-sine, sine], axis=1)

    match = matches.astype(jnp.bfloat16)

    def across(value, shift):
        pairs = [(h * HALF + i, h * HALF + (i + 2 * shift) % HALF) for h in range(2) for i in range(HALF)]
        return lax.ppermute(value, "seq", pairs)

    def spread_pieces(own, other):
        other = lax.ppermute(other, "seq", [(i, i ^ 1) for i in range(2 * HALF)])
        pairs = pair_stripes(own, other)
        near, far = [pairs[0]], []
        for s in range(1, CHIPS):
            near.append(across(pairs[s], s))
        for s in range(CHIPS):
            far.append(climb(near[s]))
        return near, far

    blended_keys, *own = blend(me, pick, match, (cosine, sine), key_rows, fresh_kv[0, :, :KV_WIDTH])
    near_keys, far_keys = spread_pieces(*own)
    blended_values, *own = blend(me, pick, match, (), value_rows, fresh_kv[0, :, KV_WIDTH:])
    near_values, far_values = spread_pieces(*own)
    blended = jnp.concatenate([blended_keys, blended_values], axis=1)

    def pieces(shifts):
        return [far_keys[s] for s in shifts] + [far_values[s] for s in shifts]

    state = attend_local(me, queries, near_keys + near_values)
    state = attend_cross(upper, queries, pieces(CLIMBS[:2]), state)
    results = {}
    for slots in (FIRST_SLOTS, LAST_SLOTS):
        results |= dict(zip(slots, attend_cross(upper, queries, pieces(CLIMBS[2:]), state, slots)))

    heads = [results[0]]
    for s in range(1, HALF):
        heads.append(turn(results[s], HALF - s))
    used = jnp.broadcast_to((chosen >= 0).astype(jnp.int32)[:, None], (SEL_DEV, 1))
    attended = place_heads(me, used, heads)
    return (blended[None], attended[None])


def solution(mesh):
    return jax.shard_map(
        on_device,
        mesh=mesh,
        in_specs=(
            P("store", "seq", None),
            P(),
            P(),
            P("store", "seq", None),
            P("store", "seq", None),
            P("store", "seq"),
        ),
        out_specs=(P("store", "seq", None), P("store", "seq", None)),
        check_vma=False,
    )
```
